32 devices in a mesh: lon: 16 (over z, x, core), lat: 2 (over y).
Axes of the slice: x: 2, y: 2, z: 4, core: 2. Of those that a mesh axis runs over, the one named last changes fastest.
Arguments:
- zonal_state: float32 [4, 32, 3, 8, 2048], P(None, None, None, 'lat', 'lon'), may hold values from -6 to 6
- zonal_courant: float32 [32, 8, 2048], P(None, 'lat', 'lon'), may hold values from -0.5 to 0.5
- zonal_length: int32 [8], P('lat'), may hold values from 512 to 2048, as said below
- zonal_owner: int32 [8, 2048], P('lat', 'lon'), may hold values from 0 to 63, as said below
- merid_state: float32 [4, 32, 3, 64, 256], P(None, None, None, 'lon', 'lat'), may hold values from -6 to 6
- merid_courant: float32 [32, 64, 256], P(None, 'lon', 'lat'), may hold values from -0.5 to 0.5
- mixing: float32 [4, 32, 32], replicated, may hold values from -0.18 to 0.18
Outputs:
- zonal_next: float32 [4, 32, 3, 8, 2048], P(None, None, None, 'lat', 'lon')
- merid_next: float32 [4, 32, 3, 64, 256], P(None, None, None, 'lon', 'lat')
- coupling: float32 [64, 8, 128], P('lon', 'lat')
The draws below stay inside these ranges and needn't reach their ends.
Inputs may be any that keep to these rules, and one draw needn't show every extreme that they name: `zonal_owner`: non-decreasing along each row; each GCM column holds 16 to 48 consecutive cells of a row, and cell x belongs to a column g with |g - x // 32| <= 1. `zonal_length`: in each latitude sector (aligned blocks of 4 cycles) the first cycle holds 1088 cells and the second 2048.
All inputs are finite; a program needn't handle non-finite values.
Results may differ from the reference program's by a relative error of at most 0.0003.
Values sent between devices are 32-bit elements; how exact they have to be, the bound alone decides.
No kernel may reach another device: no remote copies, remote signals or barrier semaphores. Data moves between devices by JAX's collectives and lax.ppermute only.
A program may use at most 64 MiB of HBM per device.

```python
import jax
import jax.numpy as jnp
from jax import lax

NV = 4
LEV = 32
WID = 3
SUB = 4
ZROWS_DEV = 4
CELLS_DEV = 128
GLON_DEV = 4
ZROWS = 8
ZCELLS = 2048
GLON = 64
MCOLS = 64
MY = 256


def draw_zonal_length(key, part):
    lengths = jax.random.randint(jax.random.fold_in(key, 5), (ZROWS,), ZCELLS // 4, ZCELLS + 1).astype(jnp.int32)
    rows = jnp.arange(ZROWS, dtype=jnp.int32)
    opposite = ZCELLS // 2 + CELLS_DEV // 2
    lengths = jnp.where(rows % ZROWS_DEV == 0, opposite, lengths)
    lengths = jnp.where(rows % ZROWS_DEV == 1, ZCELLS, lengths)
    return lengths.astype(jnp.int32)


def draw_zonal_owner(key, part):
    share = CELLS_DEV // GLON_DEV
    half = share // 2
    pairs = (GLON - 2) // 2
    shifts = jax.random.randint(jax.random.fold_in(key, 11), (ZROWS, pairs), -half, half + 1).astype(jnp.int32)
    shifts = shifts.at[0, 0].set(half)
    inner = jnp.stack([share + shifts, share - shifts], axis=-1).reshape(ZROWS, 2 * pairs)
    edge = jnp.full((ZROWS, 1), share, dtype=jnp.int32)
    widths = jnp.concatenate([edge, inner, edge], axis=1)
    ends = jnp.cumsum(widths, axis=1).astype(jnp.int32)
    cells = jnp.arange(ZCELLS, dtype=jnp.int32)

    def one_row(row_ends):
        return jnp.searchsorted(row_ends, cells, side='right').astype(jnp.int32)
    return jax.vmap(one_row)(ends).astype(jnp.int32)


def steps_of(own_key, shape, pieces, low, high):
    def one(axis_at, blocks):
        steps = jax.random.uniform(jax.random.fold_in(jax.random.fold_in(own_key, 6), axis_at), (blocks,), jnp.float32, low / len(pieces), high / len(pieces))
        return jnp.repeat(jnp.exp(steps), shape[axis_at] // blocks).reshape((-1,) + (1,) * (len(shape) - axis_at - 1))

    factor_of = one(*pieces[0])
    for cut in pieces[1:]:
        factor_of = factor_of * one(*cut)
    return factor_of


def normal_values(key, shape, deviation, bound, pieces=(), kind=jnp.bfloat16):
    entries = deviation * jax.random.normal(key, shape, jnp.float32)
    if pieces:
        entries = entries * steps_of(key, shape, pieces, -0.22, 0.18)
    return jnp.clip(entries, -bound, bound).astype(kind)


def setup_inputs(seed: int = 0) -> dict:
    key_of = jax.random.split(jax.random.key(seed), 8)
    zonal_state = normal_values(key_of[0], (NV, LEV, WID, ZROWS, ZCELLS), 1.0, 6.0, ((3, 2), (4, 16)), jnp.float32)
    zonal_courant = jnp.clip(jax.random.uniform(key_of[1], (LEV, ZROWS, ZCELLS), jnp.float32, -0.5, 0.5) * steps_of(key_of[1], (LEV, ZROWS, ZCELLS), ((1, 2), (2, 16)), -0.4, 0.0), -0.5, 0.5)
    zonal_length = draw_zonal_length(jax.random.fold_in(key_of[7], 71), 0)
    zonal_owner = draw_zonal_owner(jax.random.fold_in(key_of[7], 71), 0)
    merid_state = normal_values(key_of[4], (NV, LEV, WID, MCOLS, MY), 1.0, 6.0, ((3, 16), (4, 2)), jnp.float32)
    merid_courant = jnp.clip(jax.random.uniform(key_of[5], (LEV, MCOLS, MY), jnp.float32, -0.5, 0.5) * steps_of(key_of[5], (LEV, MCOLS, MY), ((1, 16), (2, 2)), -0.4, 0.0), -0.5, 0.5)
    mixing = normal_values(key_of[6], (NV, LEV, LEV), 0.03, 0.18, (), jnp.float32)
    return dict(zonal_state=zonal_state, zonal_courant=zonal_courant, zonal_length=zonal_length, zonal_owner=zonal_owner, merid_state=merid_state, merid_courant=merid_courant, mixing=mixing)


diffuse_along = 0.3
diffuse_across = 0.1


def across_terms(field_now):
    plus_side = jnp.concatenate([field_now[:, :, 1:], field_now[:, :, 2:3]], axis=2)
    minus_side = jnp.concatenate([field_now[:, :, 0:1], field_now[:, :, :2]], axis=2)
    return diffuse_across * (plus_side + minus_side - 2.0 * field_now)


def tendency(field_now, forward_side, backward_side, courant, mixing):
    vertical = jnp.einsum("vkj,vjwrx->vkwrx", mixing, field_now, precision=lax.Precision.HIGHEST)
    advect = -0.5 * courant * (forward_side - backward_side)
    spread = diffuse_along * (forward_side - 2.0 * field_now + backward_side)
    return advect + spread + across_terms(field_now) + vertical


def reference(zonal_state, zonal_courant, zonal_length, zonal_owner, merid_state, merid_courant, mixing):
    cells = jnp.arange(ZCELLS, dtype=jnp.int32)
    at_tail = cells[None, :] == (zonal_length[:, None] - 1)
    at_head = cells[None, :] == 0
    active = cells[None, :] < zonal_length[:, None]
    zonal_now = zonal_state
    for substep in range(SUB):
        head_cell = zonal_now[..., 0:1]
        tail_cell = jnp.sum(jnp.where(at_tail, zonal_now, 0.0), axis=-1, keepdims=True)
        forward_side = jnp.where(at_tail, head_cell, jnp.roll(zonal_now, -1, axis=-1))
        backward_side = jnp.where(at_head, tail_cell, jnp.roll(zonal_now, 1, axis=-1))
        change = tendency(zonal_now, forward_side, backward_side, zonal_courant[:, None], mixing)
        zonal_now = jnp.where(active, zonal_now + change, zonal_now)
    merid_now = merid_state
    half_turn = MCOLS // 2
    for substep in range(SUB):
        north_edge = jnp.roll(merid_now[:, :, ::-1, :, -1:], -half_turn, axis=3)
        south_edge = jnp.roll(merid_now[:, :, ::-1, :, 0:1], -half_turn, axis=3)
        forward_side = jnp.concatenate([merid_now[..., 1:], north_edge], axis=-1)
        backward_side = jnp.concatenate([south_edge, merid_now[..., :-1]], axis=-1)
        merid_now = merid_now + tendency(merid_now, forward_side, backward_side, merid_courant[:, None], mixing)
    scale = GLON_DEV / (3.0 * CELLS_DEV)
    change_sum = jnp.sum(zonal_now - zonal_state, axis=2) * scale
    flat = change_sum.reshape(NV * LEV, ZROWS, ZCELLS)
    columns = jnp.arange(GLON, dtype=jnp.int32)

    def one_row(paired):
        owner_row, change_row = paired
        onehot = (owner_row[:, None] == columns[None, :]).astype(jnp.float32)
        return jnp.einsum("xg,jx->gj", onehot, change_row, precision=lax.Precision.HIGHEST)

    rows_out = lax.map(one_row, (zonal_owner, jnp.moveaxis(flat, 1, 0)))
    coupling = jnp.transpose(rows_out, (1, 0, 2))
    return zonal_now, merid_now, coupling
```

```python
import functools

import jax
import jax.numpy as jnp
from jax import lax
from jax.experimental import pallas as pl
from jax.experimental.pallas import tpu as pltpu
from jax.sharding import PartitionSpec as P

SUB = 4
CELLS_DEV = 128
GLON_DEV = 4
DIFFUSE_ALONG = 0.3
DIFFUSE_ACROSS = 0.1
PAD = 4
CHUNK = 10


class Sizes:
    def __init__(self, state_shape):
        self.nv, self.lev, self.wid, self.rows, self.cells = state_shape
        self.lanes = self.nv * self.lev
        self.half = self.cells // 2
        self.span = self.half + 2 * SUB + 2 * PAD
        self.group = 2 * self.rows
        self.wr = self.wid * self.rows
        self.packed = self.wr + self.rows
        self.packet = SUB * self.packed


def turned_courant(sz, ref, r):
    one = ref[pl.ds(r, sz.lev, stride=sz.rows), :]
    return jnp.concatenate([one] * sz.nv, axis=0).T


def put_halves(sz, out_ref, base, r, tile_ref, at):
    n = sz.half + SUB
    first = (base + PAD + SUB) * sz.group + r
    out_ref[pl.ds(first, n, stride=sz.group), :] = tile_ref[at : at + n, :]
    second = (base + PAD) * sz.group + sz.rows + r
    out_ref[pl.ds(second, n, stride=sz.group), :] = tile_ref[
        at + sz.half - SUB : at + sz.cells, :
    ]


def turn_in(sz, lat_two, place, length, z_ref, zc_ref, m_ref, mc_ref, mix_ref,
            zt_ref, zct_ref, mt_ref, mct_ref, w_ref, zfirst, zlast, ht, htp, mlow, mhigh,
            tile, low, high):
    lon = place[0]
    lat = place[1]
    last = place[2]
    edge = 8
    tile[0:edge, :] = jnp.zeros((edge, sz.lanes), jnp.float32)
    tile[edge + sz.cells :, :] = jnp.zeros((edge, sz.lanes), jnp.float32)
    owns_head = jnp.where(lon == 0, 1.0, 0.0).astype(jnp.float32)

    def place_tile(value, slot, r, base, out_ref, zonal):
        tile[edge : edge + sz.cells, :] = value
        put_halves(sz, out_ref, base, r, tile, edge)
        at = pl.ds(slot, SUB, stride=sz.packed)
        begin = tile[edge : edge + SUB, :]
        finish = tile[edge + sz.cells - SUB : edge + sz.cells, :]
        if zonal:
            zfirst[at, :] = begin
            zlast[at, :] = finish
            offset = jnp.clip(length[r] - SUB - lon * sz.cells, -SUB, sz.cells)
            ends = tile[pl.ds(edge + offset, SUB), :]
            ht[at, :] = begin * owns_head
            ht[pl.ds(sz.packet + slot, SUB, stride=sz.packed), :] = ends
        else:
            low[at, :] = begin
            high[at, :] = finish

    for zonal, s_ref, c_ref, st_ref, ct_ref in (
        (False, m_ref, mc_ref, mt_ref, mct_ref), (True, z_ref, zc_ref, zt_ref, zct_ref)
    ):
        for r in range(sz.rows):
            for w in range(sz.wid):
                slot = w * sz.rows + r
                value = s_ref[pl.ds(slot, sz.lanes, stride=sz.wr), :].T
                place_tile(value, slot, r, w * sz.span, st_ref, zonal)
            place_tile(turned_courant(sz, c_ref, r), sz.wr + r, r, 0, ct_ref, zonal)
    htp[0 : 2 * sz.packet, :] = ht[...]
    north = jnp.where(lat == last, 1, 0)
    lows = low[...]
    highs = high[...]
    htp[2 * sz.packet :, :] = jnp.where(north == 1, highs, lows)
    if lat_two:
        mlow[...] = jnp.where(north == 1, lows, highs)
        mhigh[...] = jnp.zeros(mhigh.shape, jnp.float32)
    else:
        mlow[...] = lows
        mhigh[...] = highs
    turned = mix_ref[...].T
    full = jnp.concatenate([turned] * sz.nv, axis=0)
    shape = (sz.lanes, sz.lanes)
    source = lax.broadcasted_iota(jnp.int32, shape, 0)
    target = lax.broadcasted_iota(jnp.int32, shape, 1)
    full = jnp.where(source // sz.lev == target // sz.lev, full, 0.0)
    stay = 1.0 - 2.0 * DIFFUSE_ALONG - 2.0 * DIFFUSE_ACROSS
    full = full + jnp.where(source == target, stay, 0.0)
    coarse = full.astype(jnp.bfloat16)
    fine = (full - coarse.astype(jnp.float32)).astype(jnp.bfloat16)
    w_ref[0 : sz.lanes, 0 : sz.lanes] = coarse
    w_ref[sz.lanes :, 0 : sz.lanes] = coarse
    w_ref[0 : sz.lanes, sz.lanes :] = fine
    w_ref[sz.lanes :, sz.lanes :] = fine


def combine(count, packet, *refs):
    own, zfirst, zlast = refs[:3]
    parts = refs[3 : 3 + count]
    total_ref, first_ref, last_ref = refs[3 + count :]
    total = own[0 : 2 * packet, :]
    for part in parts:
        total = total + part[0 : 2 * packet, :]
    total_ref[...] = total
    first_ref[0 : 2 * packet, :] = total
    first_ref[2 * packet :, :] = zfirst[...]
    last_ref[0 : 2 * packet, :] = total
    last_ref[2 * packet :, :] = zlast[...]


def substeps(sz, w_ref, a_ref, b_ref, ca_ref, cb_ref, courant_ref):
    lo_y = PAD * sz.group
    rows = (sz.half + 2 * SUB) * sz.group
    c = courant_ref[lo_y : lo_y + rows, :]
    ca_ref[lo_y : lo_y + rows, :] = DIFFUSE_ALONG - 0.5 * c
    cb_ref[lo_y : lo_y + rows, :] = DIFFUSE_ALONG + 0.5 * c
    g = sz.group

    def step(src, dst):
        total = sz.half + 2 * SUB - 2
        for begin in range(0, total, CHUNK):
            size = min(CHUNK, total - begin)
            y = PAD + 1 + begin
            n = size * g
            here = [src[(w * sz.span + y) * g : (w * sz.span + y) * g + n, :] for w in range(sz.wid)]
            stacked = jnp.concatenate(here, axis=0)
            coarse = stacked.astype(jnp.bfloat16)
            fine = (stacked - coarse.astype(jnp.float32)).astype(jnp.bfloat16)
            product = jnp.dot(
                jnp.concatenate([coarse, fine], axis=1), w_ref[...],
                preferred_element_type=jnp.float32,
            )
            ca = ca_ref[y * g : y * g + n, :]
            cb = cb_ref[y * g : y * g + n, :]
            for w in range(sz.wid):
                at = (w * sz.span + y) * g
                up = here[min(w + 1, sz.wid - 1)]
                down = here[max(w - 1, 0)]
                part = product[w * n : (w + 1) * n]
                value = part[:, : sz.lanes] + part[:, sz.lanes :]
                value = value + DIFFUSE_ACROSS * (up + down)
                value = value + src[at + g : at + g + n, :] * ca
                value = value + src[at - g : at - g + n, :] * cb
                dst[at : at + n, :] = value

    def pair(_, carry):
        step(a_ref, b_ref)
        step(b_ref, a_ref)
        return carry

    lax.fori_loop(0, SUB // 2, pair, 0)


def merid_kernel(sz, lat_two, place, mt, mct, w_ref, pole, lat_a, lat_b, own_b, out_ref,
                 b_ref, ca_ref, cb_ref, ct_ref):
    lat = place[1]
    last = place[2]
    out_ref[...] = mt[...]
    ct_ref[...] = mct[...]
    base = 2 * sz.packet
    for d in range(SUB):
        for slot in range(sz.packed):
            courant = slot >= sz.wr
            w, r = divmod(slot, sz.rows)
            partner = slot if courant else (sz.wid - 1 - w) * sz.rows + r
            sign = -1.0 if courant else 1.0
            ref = ct_ref if courant else out_ref
            begin = 0 if courant else w * sz.span
            mirrored = (SUB - 1 - d) * sz.packed + partner
            over = sign * pole[base + mirrored : base + mirrored + 1, :]
            at = d * sz.packed + slot
            south = jnp.where(lat == 0, over, lat_a[at : at + 1, :])
            north = jnp.where(lat == last, over, lat_b[at : at + 1, :])
            row = (begin + PAD + d) * sz.group + r
            ref[row : row + 1, :] = south
            row = (begin + PAD + SUB + sz.half + d) * sz.group + sz.rows + r
            ref[row : row + 1, :] = north
    substeps(sz, w_ref, out_ref, b_ref, ca_ref, cb_ref, ct_ref)


def zonal_kernel(sz, shift_count, place, length, zt, zct, w_ref, owner, own, behind, ahead, *refs):
    others = refs[:shift_count]
    out_ref, near_ref, b_ref, ca_ref, cb_ref, ct_ref = refs[shift_count:]
    lon = place[0]
    out_ref[...] = zt[...]
    ct_ref[...] = zct[...]
    ends = own[...] + behind[0 : 2 * sz.packet, :] + ahead[0 : 2 * sz.packet, :]
    for other in others:
        ends = ends + other[...]
    head = ends[: sz.packet]
    left = jnp.where(lon == 0, ends[sz.packet :], behind[2 * sz.packet :, :])
    right = ahead[2 * sz.packet :, :]
    for d in range(SUB):
        for slot in range(sz.packed):
            courant = slot >= sz.wr
            w, r = divmod(slot, sz.rows)
            ref = ct_ref if courant else out_ref
            r = slot % sz.rows
            begin = 0 if courant else w * sz.span
            at = d * sz.packed + slot
            row = (begin + PAD + d) * sz.group + r
            ref[row : row + 1, :] = left[at : at + 1]
            row = (begin + PAD + SUB + sz.half + d) * sz.group + sz.rows + r
            ref[row : row + 1, :] = right[at : at + 1]
    for r in range(sz.rows):
        past = length[r] - lon * sz.cells
        for h in range(2):
            y = jnp.clip(past + PAD + SUB - h * sz.half, 0, sz.span - SUB)
            for slot in range(r, sz.packed, sz.rows):
                courant = slot >= sz.wr
                ref = ct_ref if courant else out_ref
                begin = 0 if courant else (slot // sz.rows) * sz.span
                for d in range(SUB):
                    at = d * sz.packed + slot
                    row = (begin + y + d) * sz.group + h * sz.rows + r
                    ref[pl.ds(row, 1), :] = head[at : at + 1]
    substeps(sz, w_ref, out_ref, b_ref, ca_ref, cb_ref, ct_ref)
    scale = GLON_DEV / (3.0 * CELLS_DEV)
    near = near_ref.shape[0] // sz.rows
    for r in range(sz.rows):
        column = lon * GLON_DEV - 1 + lax.broadcasted_iota(jnp.int32, (near, sz.cells), 0)
        cell = lon * sz.cells + lax.broadcasted_iota(jnp.int32, (near, sz.cells), 1)
        own_row = owner[r : r + 1, :]
        table = jnp.where((own_row == column) & (cell < length[r]), 1.0, 0.0)
        halves = []
        for h in range(2):
            change = None
            for w in range(sz.wid):
                at = pl.ds((w * sz.span + PAD + SUB) * sz.group + h * sz.rows + r,
                           sz.half, stride=sz.group)
                part = out_ref[at, :] - zt[at, :]
                change = part if change is None else change + part
            halves.append(change)
        change = jnp.concatenate(halves, axis=0) * scale
        near_ref[pl.ds(r, near, stride=sz.rows), :] = jnp.dot(
            table.astype(jnp.float32), change, precision=lax.Precision.HIGHEST,
            preferred_element_type=jnp.float32,
        )


def turn_out(sz, place, length, mt, zt, z_ref, m_out, z_out):
    lon = place[0]
    cell = lon * sz.cells + lax.broadcasted_iota(jnp.int32, (sz.lanes, sz.cells), 1)
    for zonal, src, dst in ((False, mt, m_out), (True, zt, z_out)):
        for w in range(sz.wid):
            for r in range(sz.rows):
                halves = [
                    src[pl.ds((w * sz.span + PAD + SUB) * sz.group + h * sz.rows + r,
                              sz.half, stride=sz.group), :]
                    for h in range(2)
                ]
                value = jnp.concatenate(halves, axis=0).T
                at = pl.ds(w * sz.rows + r, sz.lanes, stride=sz.wr)
                if zonal:
                    value = jnp.where(cell < length[r], value, z_ref[at, :])
                dst[at, :] = value


def call(body, outs, smem, vmem, scratch=(), name=None):
    return pl.pallas_call(
        body,
        out_shape=outs,
        in_specs=[pl.BlockSpec(memory_space=pltpu.SMEM)] * smem
        + [pl.BlockSpec(memory_space=pltpu.VMEM)] * vmem,
        out_specs=[pl.BlockSpec(memory_space=pltpu.VMEM)] * len(outs),
        scratch_shapes=list(scratch),
        name=name,
    )


def shifted(value, axis, steps):
    count = lax.axis_size(axis)
    return lax.ppermute(value, axis, [(i, (i + steps) % count) for i in range(count)])


def shards(
    zonal_state, zonal_courant, zonal_length, zonal_owner, merid_state, merid_courant, mixing
):
    sz = Sizes(zonal_state.shape)
    f32 = lambda *shape: jax.ShapeDtypeStruct(shape, jnp.float32)
    lon_count = lax.axis_size("lon")
    lat_count = lax.axis_size("lat")
    lat_two = lat_count == 2
    place = jnp.stack(
        [lax.axis_index("lon"), lax.axis_index("lat"), jnp.int32(lat_count - 1)]
    ).astype(jnp.int32)
    flat = lambda a: a.reshape(-1, sz.cells)
    z, m = flat(zonal_state), flat(merid_state)
    state_rows = sz.wid * sz.span * sz.group
    courant_rows = sz.span * sz.group
    packet = sz.packet
    lanes = sz.lanes
    zt, zct, mt, mct, weights, zfirst, zlast, ht, htp, mlow, mhigh = call(
        functools.partial(turn_in, sz, lat_two),
        (
            f32(state_rows, lanes), f32(courant_rows, lanes),
            f32(state_rows, lanes), f32(courant_rows, lanes),
            jax.ShapeDtypeStruct((2 * lanes, 2 * lanes), jnp.bfloat16),
            f32(packet, lanes), f32(packet, lanes), f32(2 * packet, lanes),
            f32(3 * packet, lanes), f32(packet, lanes), f32(packet, lanes),
        ),
        2, 5,
        (
            pltpu.VMEM((sz.cells + 16, lanes), jnp.float32),
            pltpu.VMEM((packet, lanes), jnp.float32),
            pltpu.VMEM((packet, lanes), jnp.float32),
        ),
        "turn_in",
    )(place, zonal_length, z, flat(zonal_courant), m, flat(merid_courant),
      mixing.reshape(lanes, sz.lev))
    pole = shifted(htp, "lon", lon_count // 2)
    if lat_two:
        lat_a = lat_b = shifted(mlow, "lat", 1)
    else:
        lat_b = shifted(mlow, "lat", -1)
        lat_a = shifted(mhigh, "lat", 1)
    stride = lon_count
    own = ht
    stages = []
    while stride > 4:
        radix = 4 if stride % 16 == 0 and stride != lon_count * 2 else 2
        stages.append((stride // radix, radix))
        stride //= radix
    for number, (width, radix) in enumerate(stages):
        parts = []
        for s in range(1, radix):
            if number == 0 and s * width == lon_count // 2:
                parts.append(pole)
            else:
                parts.append(shifted(own, "lon", s * width))
        own, to_left, to_right = call(
            functools.partial(combine, len(parts), packet),
            (f32(2 * packet, lanes), f32(3 * packet, lanes), f32(3 * packet, lanes)),
            0, 3 + len(parts), (), "combine",
        )(own, zfirst, zlast, *parts)
    behind = shifted(to_right, "lon", 1)
    ahead = shifted(to_left, "lon", -1)
    others = [shifted(own, "lon", s) for s in range(2, stride - 1)]
    work = (
        pltpu.VMEM((state_rows, lanes), jnp.float32),
        pltpu.VMEM((courant_rows, lanes), jnp.float32),
        pltpu.VMEM((courant_rows, lanes), jnp.float32),
        pltpu.VMEM((courant_rows, lanes), jnp.float32),
    )
    (mt_next,) = call(
        functools.partial(merid_kernel, sz, lat_two),
        (f32(state_rows, lanes),), 1, 7, work, "merid",
    )(place, mt, mct, weights, pole, lat_a, lat_b, mhigh)
    near = 8
    zt_next, near_terms = call(
        functools.partial(zonal_kernel, sz, len(others)),
        (f32(state_rows, lanes), f32(near * sz.rows, lanes)), 2, 7 + len(others), work, "zonal",
    )(place, zonal_length, zt, zct, weights, zonal_owner, own, behind, ahead, *others)
    near_terms = near_terms.reshape(near, sz.rows, lanes)
    from_right = shifted(near_terms[0], "lon", -1)
    from_left = shifted(near_terms[GLON_DEV + 1], "lon", 1)
    m_next, z_next = call(
        functools.partial(turn_out, sz),
        (f32(*m.shape), f32(*z.shape)), 2, 3, (), "turn_out",
    )(place, zonal_length, mt_next, zt_next, z)
    coupling = near_terms[1 : GLON_DEV + 1]
    coupling = jnp.concatenate(
        [coupling[:1] + from_left[None], coupling[1:-1], coupling[-1:] + from_right[None]]
    )
    return z_next.reshape(zonal_state.shape), m_next.reshape(merid_state.shape), coupling


def solution(mesh):
    return jax.shard_map(
        shards,
        mesh=mesh,
        in_specs=(
            P(None, None, None, "lat", "lon"),
            P(None, "lat", "lon"),
            P("lat"),
            P("lat", "lon"),
            P(None, None, None, "lon", "lat"),
            P(None, "lon", "lat"),
            P(),
        ),
        out_specs=(
            P(None, None, None, "lat", "lon"),
            P(None, None, None, "lon", "lat"),
            P("lon", "lat", None),
        ),
        check_vma=False,
    )
```

```python
import functools

import jax
import jax.numpy as jnp
from jax import lax
from jax.experimental import pallas as pl
from jax.experimental.pallas import tpu as pltpu
from jax.sharding import PartitionSpec as P

SUB = 4
CELLS_DEV = 128
GLON_DEV = 4
DIFFUSE_ALONG = 0.3
DIFFUSE_ACROSS = 0.1
PAD = 4
CHUNK = 10
VMEM_GRANT = 12 << 20


class Sizes:
    def __init__(self, state_shape):
        self.nv, self.lev, self.wid, self.rows, self.cells = state_shape
        self.lanes = self.nv * self.lev
        self.half = self.cells // 2
        self.span = self.half + 2 * SUB + 2 * PAD
        self.group = 2 * self.rows
        self.wr = self.wid * self.rows
        self.packed = self.wr + self.rows
        self.packet = SUB * self.packed


def turned_courant(sz, ref, r):
    one = ref[pl.ds(r, sz.lev, stride=sz.rows), :]
    return jnp.concatenate([one] * sz.nv, axis=0).T


def put_halves(sz, out_ref, base, r, tile_ref, at):
    n = sz.half + SUB
    first = (base + PAD + SUB) * sz.group + r
    out_ref[pl.ds(first, n, stride=sz.group), :] = tile_ref[at : at + n, :]
    second = (base + PAD) * sz.group + sz.rows + r
    out_ref[pl.ds(second, n, stride=sz.group), :] = tile_ref[
        at + sz.half - SUB : at + sz.cells, :
    ]


def turn_in(sz, lat_two, lat_count, length, z_ref, zc_ref, m_ref, mc_ref, mix_ref,
            zt_ref, zct_ref, mt_ref, mct_ref, w_ref, zfirst, zlast, ht, htp, mlow, mhigh,
            tile, low, high):
    lon = lax.axis_index("lon")
    lat = lax.axis_index("lat")
    last = lat_count - 1
    edge = 8
    tile[0:edge, :] = jnp.zeros((edge, sz.lanes), jnp.float32)
    tile[edge + sz.cells :, :] = jnp.zeros((edge, sz.lanes), jnp.float32)
    owns_head = jnp.where(lon == 0, 1.0, 0.0).astype(jnp.float32)

    def place_tile(value, slot, r, base, out_ref, zonal):
        tile[edge : edge + sz.cells, :] = value
        put_halves(sz, out_ref, base, r, tile, edge)
        at = pl.ds(slot, SUB, stride=sz.packed)
        begin = tile[edge : edge + SUB, :]
        finish = tile[edge + sz.cells - SUB : edge + sz.cells, :]
        if zonal:
            zfirst[at, :] = begin
            zlast[at, :] = finish
            offset = jnp.clip(length[r] - SUB - lon * sz.cells, -SUB, sz.cells)
            ends = tile[pl.ds(edge + offset, SUB), :]
            ht[at, :] = begin * owns_head
            ht[pl.ds(sz.packet + slot, SUB, stride=sz.packed), :] = ends
        else:
            low[at, :] = begin
            high[at, :] = finish

    for zonal, s_ref, c_ref, st_ref, ct_ref in (
        (False, m_ref, mc_ref, mt_ref, mct_ref), (True, z_ref, zc_ref, zt_ref, zct_ref)
    ):
        for r in range(sz.rows):
            for w in range(sz.wid):
                slot = w * sz.rows + r
                value = s_ref[pl.ds(slot, sz.lanes, stride=sz.wr), :].T
                place_tile(value, slot, r, w * sz.span, st_ref, zonal)
            place_tile(turned_courant(sz, c_ref, r), sz.wr + r, r, 0, ct_ref, zonal)
    htp[0 : 2 * sz.packet, :] = ht[...]
    north = jnp.where(lat == last, 1, 0)
    lows = low[...]
    highs = high[...]
    htp[2 * sz.packet :, :] = jnp.where(north == 1, highs, lows)
    if lat_two:
        mlow[...] = jnp.where(north == 1, lows, highs)
        mhigh[...] = jnp.zeros(mhigh.shape, jnp.float32)
    else:
        mlow[...] = lows
        mhigh[...] = highs
    turned = mix_ref[...].T
    full = jnp.concatenate([turned] * sz.nv, axis=0)
    shape = (sz.lanes, sz.lanes)
    source = lax.broadcasted_iota(jnp.int32, shape, 0)
    target = lax.broadcasted_iota(jnp.int32, shape, 1)
    full = jnp.where(source // sz.lev == target // sz.lev, full, 0.0)
    stay = 1.0 - 2.0 * DIFFUSE_ALONG - 2.0 * DIFFUSE_ACROSS
    full = full + jnp.where(source == target, stay, 0.0)
    coarse = full.astype(jnp.bfloat16)
    fine = (full - coarse.astype(jnp.float32)).astype(jnp.bfloat16)
    w_ref[0 : sz.lanes, 0 : sz.lanes] = coarse
    w_ref[sz.lanes :, 0 : sz.lanes] = coarse
    w_ref[0 : sz.lanes, sz.lanes :] = fine
    w_ref[sz.lanes :, sz.lanes :] = fine


def combine(count, packet, *refs):
    own, zfirst, zlast = refs[:3]
    parts = refs[3 : 3 + count]
    total_ref, first_ref, last_ref = refs[3 + count :]
    total = own[0 : 2 * packet, :]
    for part in parts:
        total = total + part[0 : 2 * packet, :]
    total_ref[...] = total
    first_ref[0 : 2 * packet, :] = total
    first_ref[2 * packet :, :] = zfirst[...]
    last_ref[0 : 2 * packet, :] = total
    last_ref[2 * packet :, :] = zlast[...]


def substeps(sz, w_ref, a_ref, b_ref, ca_ref, cb_ref, courant_ref):
    lo_y = PAD * sz.group
    rows = (sz.half + 2 * SUB) * sz.group
    c = courant_ref[lo_y : lo_y + rows, :]
    ca_ref[lo_y : lo_y + rows, :] = DIFFUSE_ALONG - 0.5 * c
    cb_ref[lo_y : lo_y + rows, :] = DIFFUSE_ALONG + 0.5 * c
    g = sz.group

    def step(src, dst):
        total = sz.half + 2 * SUB - 2
        for begin in range(0, total, CHUNK):
            size = min(CHUNK, total - begin)
            y = PAD + 1 + begin
            n = size * g
            here = [src[(w * sz.span + y) * g : (w * sz.span + y) * g + n, :] for w in range(sz.wid)]
            stacked = jnp.concatenate(here, axis=0)
            coarse = stacked.astype(jnp.bfloat16)
            fine = (stacked - coarse.astype(jnp.float32)).astype(jnp.bfloat16)
            product = jnp.dot(
                jnp.concatenate([coarse, fine], axis=1), w_ref[...],
                preferred_element_type=jnp.float32,
            )
            ca = ca_ref[y * g : y * g + n, :]
            cb = cb_ref[y * g : y * g + n, :]
            for w in range(sz.wid):
                at = (w * sz.span + y) * g
                up = here[min(w + 1, sz.wid - 1)]
                down = here[max(w - 1, 0)]
                part = product[w * n : (w + 1) * n]
                value = part[:, : sz.lanes] + part[:, sz.lanes :]
                value = value + DIFFUSE_ACROSS * (up + down)
                value = value + src[at + g : at + g + n, :] * ca
                value = value + src[at - g : at - g + n, :] * cb
                dst[at : at + n, :] = value

    def pair(_, carry):
        step(a_ref, b_ref)
        step(b_ref, a_ref)
        return carry

    lax.fori_loop(0, SUB // 2, pair, 0)


def merid_kernel(sz, lat_two, lat_count, mt, mct, w_ref, pole, lat_a, lat_b, own_b, out_ref,
                 b_ref, ca_ref, cb_ref, ct_ref):
    lat = lax.axis_index("lat")
    last = lat_count - 1
    out_ref[...] = mt[...]
    ct_ref[...] = mct[...]
    base = 2 * sz.packet
    for d in range(SUB):
        for slot in range(sz.packed):
            courant = slot >= sz.wr
            w, r = divmod(slot, sz.rows)
            partner = slot if courant else (sz.wid - 1 - w) * sz.rows + r
            sign = -1.0 if courant else 1.0
            ref = ct_ref if courant else out_ref
            begin = 0 if courant else w * sz.span
            mirrored = (SUB - 1 - d) * sz.packed + partner
            over = sign * pole[base + mirrored : base + mirrored + 1, :]
            at = d * sz.packed + slot
            south = jnp.where(lat == 0, over, lat_a[at : at + 1, :])
            north = jnp.where(lat == last, over, lat_b[at : at + 1, :])
            row = (begin + PAD + d) * sz.group + r
            ref[row : row + 1, :] = south
            row = (begin + PAD + SUB + sz.half + d) * sz.group + sz.rows + r
            ref[row : row + 1, :] = north
    substeps(sz, w_ref, out_ref, b_ref, ca_ref, cb_ref, ct_ref)


def zonal_kernel(sz, shift_count, length, zt, zct, w_ref, owner, own, behind, ahead, *refs):
    others = refs[:shift_count]
    out_ref, below_ref, mid_ref, above_ref, b_ref, ca_ref, cb_ref, ct_ref = refs[shift_count:]
    lon = lax.axis_index("lon")
    out_ref[...] = zt[...]
    ct_ref[...] = zct[...]
    ends = own[...] + behind[0 : 2 * sz.packet, :] + ahead[0 : 2 * sz.packet, :]
    for other in others:
        ends = ends + other[...]
    head = ends[: sz.packet]
    left = jnp.where(lon == 0, ends[sz.packet :], behind[2 * sz.packet :, :])
    right = ahead[2 * sz.packet :, :]
    for d in range(SUB):
        for slot in range(sz.packed):
            courant = slot >= sz.wr
            w, r = divmod(slot, sz.rows)
            ref = ct_ref if courant else out_ref
            r = slot % sz.rows
            begin = 0 if courant else w * sz.span
            at = d * sz.packed + slot
            row = (begin + PAD + d) * sz.group + r
            ref[row : row + 1, :] = left[at : at + 1]
            row = (begin + PAD + SUB + sz.half + d) * sz.group + sz.rows + r
            ref[row : row + 1, :] = right[at : at + 1]
    for r in range(sz.rows):
        past = length[r] - lon * sz.cells
        for h in range(2):
            y = jnp.clip(past + PAD + SUB - h * sz.half, 0, sz.span - SUB)
            for slot in range(r, sz.packed, sz.rows):
                courant = slot >= sz.wr
                ref = ct_ref if courant else out_ref
                begin = 0 if courant else (slot // sz.rows) * sz.span
                for d in range(SUB):
                    at = d * sz.packed + slot
                    row = (begin + y + d) * sz.group + h * sz.rows + r
                    ref[pl.ds(row, 1), :] = head[at : at + 1]
    substeps(sz, w_ref, out_ref, b_ref, ca_ref, cb_ref, ct_ref)
    scale = GLON_DEV / (3.0 * CELLS_DEV)
    near = 8
    for r in range(sz.rows):
        column = lon * GLON_DEV - 1 + lax.broadcasted_iota(jnp.int32, (near, sz.cells), 0)
        cell = lon * sz.cells + lax.broadcasted_iota(jnp.int32, (near, sz.cells), 1)
        own_row = owner[r : r + 1, :]
        table = jnp.where((own_row == column) & (cell < length[r]), 1.0, 0.0)
        halves = []
        for h in range(2):
            change = None
            for w in range(sz.wid):
                at = pl.ds((w * sz.span + PAD + SUB) * sz.group + h * sz.rows + r,
                           sz.half, stride=sz.group)
                part = out_ref[at, :] - zt[at, :]
                change = part if change is None else change + part
            halves.append(change)
        change = jnp.concatenate(halves, axis=0) * scale
        sums = jnp.dot(
            table.astype(jnp.float32), change, precision=lax.Precision.HIGHEST,
            preferred_element_type=jnp.float32,
        )
        below_ref[r : r + 1, :] = sums[0:1]
        above_ref[r : r + 1, :] = sums[GLON_DEV + 1 : GLON_DEV + 2]
        for g in range(GLON_DEV):
            mid_ref[g * sz.rows + r : g * sz.rows + r + 1, :] = sums[g + 1 : g + 2]


def turn_out(sz, length, mt, zt, z_ref, m_out, z_out):
    lon = lax.axis_index("lon")
    cell = lon * sz.cells + lax.broadcasted_iota(jnp.int32, (sz.lanes, sz.cells), 1)
    for zonal, src, dst in ((False, mt, m_out), (True, zt, z_out)):
        for w in range(sz.wid):
            for r in range(sz.rows):
                halves = [
                    src[pl.ds((w * sz.span + PAD + SUB) * sz.group + h * sz.rows + r,
                              sz.half, stride=sz.group), :]
                    for h in range(2)
                ]
                value = jnp.concatenate(halves, axis=0).T
                at = pl.ds(w * sz.rows + r, sz.lanes, stride=sz.wr)
                if zonal:
                    value = jnp.where(cell < length[r], value, z_ref[at, :])
                dst[at, :] = value


def finish(sz, mid, from_left, from_right, out_ref):
    end = (GLON_DEV - 1) * sz.rows
    out_ref[0 : sz.rows, :] = mid[0 : sz.rows, :] + from_left[...]
    out_ref[sz.rows : end, :] = mid[sz.rows : end, :]
    out_ref[end:, :] = mid[end:, :] + from_right[...]


def call(body, outs, smem, vmem, scratch=(), name=None, flops=1 << 20):
    return pl.pallas_call(
        body,
        out_shape=outs,
        in_specs=[pl.BlockSpec(memory_space=pltpu.SMEM)] * smem
        + [pl.BlockSpec(memory_space=pltpu.VMEM)] * vmem,
        out_specs=[pl.BlockSpec(memory_space=pltpu.VMEM)] * len(outs),
        scratch_shapes=list(scratch),
        compiler_params=pltpu.CompilerParams(vmem_limit_bytes=VMEM_GRANT),
        cost_estimate=pl.CostEstimate(flops=flops, bytes_accessed=4 << 20, transcendentals=0),
        name=name,
    )


def shifted(value, axis, steps):
    count = lax.axis_size(axis)
    return lax.ppermute(value, axis, [(i, (i + steps) % count) for i in range(count)])


def shards(
    zonal_state, zonal_courant, zonal_length, zonal_owner, merid_state, merid_courant, mixing
):
    sz = Sizes(zonal_state.shape)
    f32 = lambda *shape: jax.ShapeDtypeStruct(shape, jnp.float32)
    lon_count = lax.axis_size("lon")
    lat_count = lax.axis_size("lat")
    lat_two = lat_count == 2
    flat = lambda a: a.reshape(-1, sz.cells)
    z, m = flat(zonal_state), flat(merid_state)
    state_rows = sz.wid * sz.span * sz.group
    courant_rows = sz.span * sz.group
    packet = sz.packet
    lanes = sz.lanes
    zt, zct, mt, mct, weights, zfirst, zlast, ht, htp, mlow, mhigh = call(
        functools.partial(turn_in, sz, lat_two, lat_count),
        (
            f32(state_rows, lanes), f32(courant_rows, lanes),
            f32(state_rows, lanes), f32(courant_rows, lanes),
            jax.ShapeDtypeStruct((2 * lanes, 2 * lanes), jnp.bfloat16),
            f32(packet, lanes), f32(packet, lanes), f32(2 * packet, lanes),
            f32(3 * packet, lanes), f32(packet, lanes), f32(packet, lanes),
        ),
        1, 5,
        (
            pltpu.VMEM((sz.cells + 16, lanes), jnp.float32),
            pltpu.VMEM((packet, lanes), jnp.float32),
            pltpu.VMEM((packet, lanes), jnp.float32),
        ),
        "turn_in",
    )(zonal_length, z, flat(zonal_courant), m, flat(merid_courant),
      mixing.reshape(lanes, sz.lev))
    pole = shifted(htp, "lon", lon_count // 2)
    if lat_two:
        lat_a = lat_b = shifted(mlow, "lat", 1)
    else:
        lat_b = shifted(mlow, "lat", -1)
        lat_a = shifted(mhigh, "lat", 1)
    stride = lon_count
    own = ht
    stages = []
    while stride > 4:
        radix = 4 if stride % 16 == 0 and stride != lon_count * 2 else 2
        stages.append((stride // radix, radix))
        stride //= radix
    for number, (width, radix) in enumerate(stages):
        parts = []
        for s in range(1, radix):
            if number == 0 and s * width == lon_count // 2:
                parts.append(pole)
            else:
                parts.append(shifted(own, "lon", s * width))
        own, to_left, to_right = call(
            functools.partial(combine, len(parts), packet),
            (f32(2 * packet, lanes), f32(3 * packet, lanes), f32(3 * packet, lanes)),
            0, 3 + len(parts), (), "combine",
        )(own, zfirst, zlast, *parts)
    behind = shifted(to_right, "lon", 1)
    ahead = shifted(to_left, "lon", -1)
    others = [shifted(own, "lon", s) for s in range(2, stride - 1)]
    work = (
        pltpu.VMEM((state_rows, lanes), jnp.float32),
        pltpu.VMEM((courant_rows, lanes), jnp.float32),
        pltpu.VMEM((courant_rows, lanes), jnp.float32),
        pltpu.VMEM((courant_rows, lanes), jnp.float32),
    )
    (mt_next,) = call(
        functools.partial(merid_kernel, sz, lat_two, lat_count),
        (f32(state_rows, lanes),), 0, 7, work, "merid", 1 << 32,
    )(mt, mct, weights, pole, lat_a, lat_b, mhigh)
    own, mt_next = lax.optimization_barrier((own, mt_next))
    zt_next, below, mid, above = call(
        functools.partial(zonal_kernel, sz, len(others)),
        (
            f32(state_rows, lanes), f32(sz.rows, lanes), f32(GLON_DEV * sz.rows, lanes),
            f32(sz.rows, lanes),
        ),
        1, 7 + len(others), work, "zonal", 1 << 32,
    )(zonal_length, zt, zct, weights, zonal_owner, own, behind, ahead, *others)
    from_right = shifted(below, "lon", -1)
    from_left = shifted(above, "lon", 1)
    m_next, z_next = call(
        functools.partial(turn_out, sz),
        (f32(*m.shape), f32(*z.shape)), 1, 3, (), "turn_out", 1 << 32,
    )(zonal_length, mt_next, zt_next, z)
    (coupling,) = call(
        functools.partial(finish, sz), (f32(*mid.shape),), 0, 3, (), "finish",
    )(mid, from_left, from_right)
    coupling = coupling.reshape(GLON_DEV, sz.rows, lanes)
    return z_next.reshape(zonal_state.shape), m_next.reshape(merid_state.shape), coupling


def solution(mesh):
    return jax.shard_map(
        shards,
        mesh=mesh,
        in_specs=(
            P(None, None, None, "lat", "lon"),
            P(None, "lat", "lon"),
            P("lat"),
            P("lat", "lon"),
            P(None, None, None, "lon", "lat"),
            P(None, "lon", "lat"),
            P(),
        ),
        out_specs=(
            P(None, None, None, "lat", "lon"),
            P(None, None, None, "lon", "lat"),
            P("lon", "lat", None),
        ),
        check_vma=False,
    )
```

```python
import functools

import jax
import jax.numpy as jnp
from jax import lax
from jax.experimental import pallas as pl
from jax.experimental.pallas import tpu as pltpu
from jax.sharding import PartitionSpec as P

SUB = 4
CELLS_DEV = 128
GLON_DEV = 4
DIFFUSE_ALONG = 0.3
DIFFUSE_ACROSS = 0.1
PAD = 4
CHUNK = 10
VMEM_GRANT = 12 << 20


class Sizes:
    def __init__(self, state_shape):
        self.nv, self.lev, self.wid, self.rows, self.cells = state_shape
        self.lanes = self.nv * self.lev
        self.half = self.cells // 2
        self.span = self.half + 2 * SUB + 2 * PAD
        self.group = 2 * self.rows
        self.wr = self.wid * self.rows
        self.packed = self.wr + self.rows
        self.packet = SUB * self.packed


def turned_courant(sz, ref, r):
    one = ref[pl.ds(r, sz.lev, stride=sz.rows), :]
    return jnp.concatenate([one] * sz.nv, axis=0).T


def put_halves(sz, out_ref, base, r, tile_ref, at):
    n = sz.half + SUB
    first = (base + PAD + SUB) * sz.group + r
    out_ref[pl.ds(first, n, stride=sz.group), :] = tile_ref[at : at + n, :]
    second = (base + PAD) * sz.group + sz.rows + r
    out_ref[pl.ds(second, n, stride=sz.group), :] = tile_ref[
        at + sz.half - SUB : at + sz.cells, :
    ]


def turn_in(sz, lat_two, lat_count, length_ref, z_ref, zc_ref, m_ref, mc_ref, mix_ref,
            zt_ref, zct_ref, mt_ref, mct_ref, w_ref, zfirst, zlast, ht, htp, mlow, mhigh,
            tile, low, high, z_in, zc_in, m_in, mc_in, mix_in, length, sems):
    copies = [
        pltpu.make_async_copy(source, target, sems.at[n])
        for n, (source, target) in enumerate((
            (length_ref, length), (m_ref, m_in), (mc_ref, mc_in), (z_ref, z_in),
            (zc_ref, zc_in), (mix_ref, mix_in),
        ))
    ]
    for copy in copies:
        copy.start()
    lon = lax.axis_index("lon")
    lat = lax.axis_index("lat")
    last = lat_count - 1
    edge = 8
    tile[0:edge, :] = jnp.zeros((edge, sz.lanes), jnp.float32)
    tile[edge + sz.cells :, :] = jnp.zeros((edge, sz.lanes), jnp.float32)
    owns_head = jnp.where(lon == 0, 1.0, 0.0).astype(jnp.float32)

    def place_tile(value, slot, r, base, out_ref, zonal):
        tile[edge : edge + sz.cells, :] = value
        put_halves(sz, out_ref, base, r, tile, edge)
        at = pl.ds(slot, SUB, stride=sz.packed)
        begin = tile[edge : edge + SUB, :]
        finish = tile[edge + sz.cells - SUB : edge + sz.cells, :]
        if zonal:
            zfirst[at, :] = begin
            zlast[at, :] = finish
            offset = jnp.clip(length[r] - SUB - lon * sz.cells, -SUB, sz.cells)
            ends = tile[pl.ds(edge + offset, SUB), :]
            ht[at, :] = begin * owns_head
            ht[pl.ds(sz.packet + slot, SUB, stride=sz.packed), :] = ends
        else:
            low[at, :] = begin
            high[at, :] = finish

    for zonal, s_ref, c_ref, st_ref, ct_ref in (
        (False, m_in, mc_in, mt_ref, mct_ref), (True, z_in, zc_in, zt_ref, zct_ref)
    ):
        if zonal:
            copies[0].wait()
            copies[3].wait()
            copies[4].wait()
        else:
            copies[1].wait()
            copies[2].wait()
        for r in range(sz.rows):
            for w in range(sz.wid):
                slot = w * sz.rows + r
                value = s_ref[pl.ds(slot, sz.lanes, stride=sz.wr), :].T
                place_tile(value, slot, r, w * sz.span, st_ref, zonal)
            place_tile(turned_courant(sz, c_ref, r), sz.wr + r, r, 0, ct_ref, zonal)
    htp[0 : 2 * sz.packet, :] = ht[...]
    north = jnp.where(lat == last, 1, 0)
    lows = low[...]
    highs = high[...]
    htp[2 * sz.packet :, :] = jnp.where(north == 1, highs, lows)
    if lat_two:
        mlow[...] = jnp.where(north == 1, lows, highs)
        mhigh[...] = jnp.zeros(mhigh.shape, jnp.float32)
    else:
        mlow[...] = lows
        mhigh[...] = highs
    copies[5].wait()
    turned = mix_in[...].T
    full = jnp.concatenate([turned] * sz.nv, axis=0)
    shape = (sz.lanes, sz.lanes)
    source = lax.broadcasted_iota(jnp.int32, shape, 0)
    target = lax.broadcasted_iota(jnp.int32, shape, 1)
    full = jnp.where(source // sz.lev == target // sz.lev, full, 0.0)
    stay = 1.0 - 2.0 * DIFFUSE_ALONG - 2.0 * DIFFUSE_ACROSS
    full = full + jnp.where(source == target, stay, 0.0)
    coarse = full.astype(jnp.bfloat16)
    fine = (full - coarse.astype(jnp.float32)).astype(jnp.bfloat16)
    w_ref[0 : sz.lanes, 0 : sz.lanes] = coarse
    w_ref[sz.lanes :, 0 : sz.lanes] = coarse
    w_ref[0 : sz.lanes, sz.lanes :] = fine
    w_ref[sz.lanes :, sz.lanes :] = fine


def combine(count, packet, *refs):
    own, zfirst, zlast = refs[:3]
    parts = refs[3 : 3 + count]
    total_ref, first_ref, last_ref = refs[3 + count :]
    total = own[0 : 2 * packet, :]
    for part in parts:
        total = total + part[0 : 2 * packet, :]
    total_ref[...] = total
    first_ref[0 : 2 * packet, :] = total
    first_ref[2 * packet :, :] = zfirst[...]
    last_ref[0 : 2 * packet, :] = total
    last_ref[2 * packet :, :] = zlast[...]


def substeps(sz, w_ref, a_ref, b_ref, ca_ref, cb_ref, courant_ref):
    lo_y = PAD * sz.group
    rows = (sz.half + 2 * SUB) * sz.group
    c = courant_ref[lo_y : lo_y + rows, :]
    ca_ref[lo_y : lo_y + rows, :] = DIFFUSE_ALONG - 0.5 * c
    cb_ref[lo_y : lo_y + rows, :] = DIFFUSE_ALONG + 0.5 * c
    g = sz.group

    def step(src, dst):
        total = sz.half + 2 * SUB - 2
        for begin in range(0, total, CHUNK):
            size = min(CHUNK, total - begin)
            y = PAD + 1 + begin
            n = size * g
            here = [src[(w * sz.span + y) * g : (w * sz.span + y) * g + n, :] for w in range(sz.wid)]
            stacked = jnp.concatenate(here, axis=0)
            coarse = stacked.astype(jnp.bfloat16)
            fine = (stacked - coarse.astype(jnp.float32)).astype(jnp.bfloat16)
            product = jnp.dot(
                jnp.concatenate([coarse, fine], axis=1), w_ref[...],
                preferred_element_type=jnp.float32,
            )
            ca = ca_ref[y * g : y * g + n, :]
            cb = cb_ref[y * g : y * g + n, :]
            for w in range(sz.wid):
                at = (w * sz.span + y) * g
                up = here[min(w + 1, sz.wid - 1)]
                down = here[max(w - 1, 0)]
                part = product[w * n : (w + 1) * n]
                value = part[:, : sz.lanes] + part[:, sz.lanes :]
                value = value + DIFFUSE_ACROSS * (up + down)
                value = value + src[at + g : at + g + n, :] * ca
                value = value + src[at - g : at - g + n, :] * cb
                dst[at : at + n, :] = value

    def pair(_, carry):
        step(a_ref, b_ref)
        step(b_ref, a_ref)
        return carry

    lax.fori_loop(0, SUB // 2, pair, 0)


def merid_kernel(sz, lat_two, lat_count, mt, mct, w_ref, pole, lat_a, lat_b, own_b, out_ref,
                 b_ref, ca_ref, cb_ref, ct_ref):
    lat = lax.axis_index("lat")
    last = lat_count - 1
    out_ref[...] = mt[...]
    ct_ref[...] = mct[...]
    base = 2 * sz.packet
    for d in range(SUB):
        for slot in range(sz.packed):
            courant = slot >= sz.wr
            w, r = divmod(slot, sz.rows)
            partner = slot if courant else (sz.wid - 1 - w) * sz.rows + r
            sign = -1.0 if courant else 1.0
            ref = ct_ref if courant else out_ref
            begin = 0 if courant else w * sz.span
            mirrored = (SUB - 1 - d) * sz.packed + partner
            over = sign * pole[base + mirrored : base + mirrored + 1, :]
            at = d * sz.packed + slot
            south = jnp.where(lat == 0, over, lat_a[at : at + 1, :])
            north = jnp.where(lat == last, over, lat_b[at : at + 1, :])
            row = (begin + PAD + d) * sz.group + r
            ref[row : row + 1, :] = south
            row = (begin + PAD + SUB + sz.half + d) * sz.group + sz.rows + r
            ref[row : row + 1, :] = north
    substeps(sz, w_ref, out_ref, b_ref, ca_ref, cb_ref, ct_ref)


def zonal_kernel(sz, shift_count, length_ref, owner_ref, zt, zct, w_ref, own, behind, ahead, *refs):
    others = refs[:shift_count]
    out_ref, below_ref, mid_ref, above_ref, b_ref, ca_ref, cb_ref, ct_ref, length, owner, sems = (
        refs[shift_count:]
    )
    copies = [
        pltpu.make_async_copy(length_ref, length, sems.at[0]),
        pltpu.make_async_copy(owner_ref, owner, sems.at[1]),
    ]
    for copy in copies:
        copy.start()
    lon = lax.axis_index("lon")
    out_ref[...] = zt[...]
    ct_ref[...] = zct[...]
    ends = own[...] + behind[0 : 2 * sz.packet, :] + ahead[0 : 2 * sz.packet, :]
    for other in others:
        ends = ends + other[...]
    head = ends[: sz.packet]
    left = jnp.where(lon == 0, ends[sz.packet :], behind[2 * sz.packet :, :])
    right = ahead[2 * sz.packet :, :]
    for d in range(SUB):
        for slot in range(sz.packed):
            courant = slot >= sz.wr
            w, r = divmod(slot, sz.rows)
            ref = ct_ref if courant else out_ref
            r = slot % sz.rows
            begin = 0 if courant else w * sz.span
            at = d * sz.packed + slot
            row = (begin + PAD + d) * sz.group + r
            ref[row : row + 1, :] = left[at : at + 1]
            row = (begin + PAD + SUB + sz.half + d) * sz.group + sz.rows + r
            ref[row : row + 1, :] = right[at : at + 1]
    copies[0].wait()
    for r in range(sz.rows):
        past = length[r] - lon * sz.cells
        for h in range(2):
            y = jnp.clip(past + PAD + SUB - h * sz.half, 0, sz.span - SUB)
            for slot in range(r, sz.packed, sz.rows):
                courant = slot >= sz.wr
                ref = ct_ref if courant else out_ref
                begin = 0 if courant else (slot // sz.rows) * sz.span
                for d in range(SUB):
                    at = d * sz.packed + slot
                    row = (begin + y + d) * sz.group + h * sz.rows + r
                    ref[pl.ds(row, 1), :] = head[at : at + 1]
    substeps(sz, w_ref, out_ref, b_ref, ca_ref, cb_ref, ct_ref)
    scale = GLON_DEV / (3.0 * CELLS_DEV)
    near = 8
    copies[1].wait()
    for r in range(sz.rows):
        column = lon * GLON_DEV - 1 + lax.broadcasted_iota(jnp.int32, (near, sz.cells), 0)
        cell = lon * sz.cells + lax.broadcasted_iota(jnp.int32, (near, sz.cells), 1)
        own_row = owner[r : r + 1, :]
        table = jnp.where((own_row == column) & (cell < length[r]), 1.0, 0.0)
        halves = []
        for h in range(2):
            change = None
            for w in range(sz.wid):
                at = pl.ds((w * sz.span + PAD + SUB) * sz.group + h * sz.rows + r,
                           sz.half, stride=sz.group)
                part = out_ref[at, :] - zt[at, :]
                change = part if change is None else change + part
            halves.append(change)
        change = jnp.concatenate(halves, axis=0) * scale
        sums = jnp.dot(
            table.astype(jnp.float32), change, precision=lax.Precision.HIGHEST,
            preferred_element_type=jnp.float32,
        )
        below_ref[r : r + 1, :] = sums[0:1]
        above_ref[r : r + 1, :] = sums[GLON_DEV + 1 : GLON_DEV + 2]
        for g in range(GLON_DEV):
            mid_ref[g * sz.rows + r : g * sz.rows + r + 1, :] = sums[g + 1 : g + 2]


def turn_out(sz, length_ref, z_ref, mt, zt, m_out, z_out, m_own, z_own, z_in, length, sems):
    reads = [
        pltpu.make_async_copy(length_ref, length, sems.at[0]),
        pltpu.make_async_copy(z_ref, z_in, sems.at[1]),
    ]
    for copy in reads:
        copy.start()
    writes = []
    lon = lax.axis_index("lon")
    cell = lon * sz.cells + lax.broadcasted_iota(jnp.int32, (sz.lanes, sz.cells), 1)
    for zonal, src, dst, out in ((False, mt, m_own, m_out), (True, zt, z_own, z_out)):
        if zonal:
            for copy in reads:
                copy.wait()
        for w in range(sz.wid):
            for r in range(sz.rows):
                halves = [
                    src[pl.ds((w * sz.span + PAD + SUB) * sz.group + h * sz.rows + r,
                              sz.half, stride=sz.group), :]
                    for h in range(2)
                ]
                value = jnp.concatenate(halves, axis=0).T
                at = pl.ds(w * sz.rows + r, sz.lanes, stride=sz.wr)
                if zonal:
                    value = jnp.where(cell < length[r], value, z_in[at, :])
                dst[at, :] = value
        writes.append(pltpu.make_async_copy(dst, out, sems.at[2 + zonal]))
        writes[-1].start()
    for copy in writes:
        copy.wait()


def finish(sz, mid, from_left, from_right, out_ref):
    end = (GLON_DEV - 1) * sz.rows
    out_ref[0 : sz.rows, :] = mid[0 : sz.rows, :] + from_left[...]
    out_ref[sz.rows : end, :] = mid[sz.rows : end, :]
    out_ref[end:, :] = mid[end:, :] + from_right[...]


def call(body, outs, spaces, scratch=(), name=None, flops=1 << 20, out_space=pltpu.VMEM):
    return pl.pallas_call(
        body,
        out_shape=outs,
        in_specs=[pl.BlockSpec(memory_space=space) for space in spaces],
        out_specs=[pl.BlockSpec(memory_space=out_space)] * len(outs),
        scratch_shapes=list(scratch),
        compiler_params=pltpu.CompilerParams(vmem_limit_bytes=VMEM_GRANT),
        cost_estimate=pl.CostEstimate(flops=flops, bytes_accessed=4 << 20, transcendentals=0),
        name=name,
    )


def shifted(value, axis, steps):
    count = lax.axis_size(axis)
    return lax.ppermute(value, axis, [(i, (i + steps) % count) for i in range(count)])


def shards(
    zonal_state, zonal_courant, zonal_length, zonal_owner, merid_state, merid_courant, mixing
):
    sz = Sizes(zonal_state.shape)
    zonal_length = pltpu.with_memory_space_constraint(zonal_length, pltpu.HBM)
    f32 = lambda *shape: jax.ShapeDtypeStruct(shape, jnp.float32)
    lon_count = lax.axis_size("lon")
    lat_count = lax.axis_size("lat")
    lat_two = lat_count == 2
    flat = lambda a: a.reshape(-1, sz.cells)
    hbm = lambda a: pltpu.with_memory_space_constraint(a, pltpu.HBM)
    z, m = hbm(flat(zonal_state)), hbm(flat(merid_state))
    state_rows = sz.wid * sz.span * sz.group
    courant_rows = sz.span * sz.group
    packet = sz.packet
    lanes = sz.lanes
    zt, zct, mt, mct, weights, zfirst, zlast, ht, htp, mlow, mhigh = call(
        functools.partial(turn_in, sz, lat_two, lat_count),
        (
            f32(state_rows, lanes), f32(courant_rows, lanes),
            f32(state_rows, lanes), f32(courant_rows, lanes),
            jax.ShapeDtypeStruct((2 * lanes, 2 * lanes), jnp.bfloat16),
            f32(packet, lanes), f32(packet, lanes), f32(2 * packet, lanes),
            f32(3 * packet, lanes), f32(packet, lanes), f32(packet, lanes),
        ),
        [pltpu.HBM] * 6,
        (
            pltpu.VMEM((sz.cells + 16, lanes), jnp.float32),
            pltpu.VMEM((packet, lanes), jnp.float32),
            pltpu.VMEM((packet, lanes), jnp.float32),
            pltpu.VMEM(z.shape, jnp.float32),
            pltpu.VMEM((sz.lev * sz.rows, sz.cells), jnp.float32),
            pltpu.VMEM(m.shape, jnp.float32),
            pltpu.VMEM((sz.lev * sz.rows, sz.cells), jnp.float32),
            pltpu.VMEM((lanes, sz.lev), jnp.float32),
            pltpu.SMEM((sz.rows,), jnp.int32),
            pltpu.SemaphoreType.DMA((6,)),
        ),
        "turn_in",
    )(zonal_length, z, hbm(flat(zonal_courant)), m, hbm(flat(merid_courant)),
      hbm(mixing.reshape(lanes, sz.lev)))
    pole = shifted(htp, "lon", lon_count // 2)
    if lat_two:
        lat_a = lat_b = shifted(mlow, "lat", 1)
    else:
        lat_b = shifted(mlow, "lat", -1)
        lat_a = shifted(mhigh, "lat", 1)
    stride = lon_count
    own = ht
    stages = []
    while stride > 4:
        radix = 4 if stride % 16 == 0 and stride != lon_count * 2 else 2
        stages.append((stride // radix, radix))
        stride //= radix
    for number, (width, radix) in enumerate(stages):
        parts = []
        for s in range(1, radix):
            if number == 0 and s * width == lon_count // 2:
                parts.append(pole)
            else:
                parts.append(shifted(own, "lon", s * width))
        own, to_left, to_right = call(
            functools.partial(combine, len(parts), packet),
            (f32(2 * packet, lanes), f32(3 * packet, lanes), f32(3 * packet, lanes)),
            [pltpu.VMEM] * (3 + len(parts)), (), "combine",
        )(own, zfirst, zlast, *parts)
    behind = shifted(to_right, "lon", 1)
    ahead = shifted(to_left, "lon", -1)
    others = [shifted(own, "lon", s) for s in range(2, stride - 1)]
    work = (
        pltpu.VMEM((state_rows, lanes), jnp.float32),
        pltpu.VMEM((courant_rows, lanes), jnp.float32),
        pltpu.VMEM((courant_rows, lanes), jnp.float32),
        pltpu.VMEM((courant_rows, lanes), jnp.float32),
    )
    (mt_next,) = call(
        functools.partial(merid_kernel, sz, lat_two, lat_count),
        (f32(state_rows, lanes),), [pltpu.VMEM] * 7, work, "merid", 1 << 32,
    )(mt, mct, weights, pole, lat_a, lat_b, mhigh)
    own, mt_next = lax.optimization_barrier((own, mt_next))
    zt_next, below, mid, above = call(
        functools.partial(zonal_kernel, sz, len(others)),
        (
            f32(state_rows, lanes), f32(sz.rows, lanes), f32(GLON_DEV * sz.rows, lanes),
            f32(sz.rows, lanes),
        ),
        [pltpu.HBM] * 2 + [pltpu.VMEM] * (6 + len(others)),
        work + (
            pltpu.SMEM((sz.rows,), jnp.int32),
            pltpu.VMEM((sz.rows, sz.cells), jnp.int32),
            pltpu.SemaphoreType.DMA((2,)),
        ),
        "zonal", 1 << 32,
    )(zonal_length, zonal_owner, zt, zct, weights, own, behind, ahead, *others)
    from_right = shifted(below, "lon", -1)
    from_left = shifted(above, "lon", 1)
    m_next, z_next = call(
        functools.partial(turn_out, sz),
        (f32(*m.shape), f32(*z.shape)), [pltpu.HBM] * 2 + [pltpu.VMEM] * 2,
        (
            pltpu.VMEM(m.shape, jnp.float32), pltpu.VMEM(z.shape, jnp.float32),
            pltpu.VMEM(z.shape, jnp.float32), pltpu.SMEM((sz.rows,), jnp.int32),
            pltpu.SemaphoreType.DMA((4,)),
        ),
        "turn_out", 1 << 32, pltpu.HBM,
    )(zonal_length, z, mt_next, zt_next)
    (coupling,) = call(
        functools.partial(finish, sz), (f32(*mid.shape),), [pltpu.VMEM] * 3, (), "finish",
    )(mid, from_left, from_right)
    coupling = coupling.reshape(GLON_DEV, sz.rows, lanes)
    return z_next.reshape(zonal_state.shape), m_next.reshape(merid_state.shape), coupling


def solution(mesh):
    return jax.shard_map(
        shards,
        mesh=mesh,
        in_specs=(
            P(None, None, None, "lat", "lon"),
            P(None, "lat", "lon"),
            P("lat"),
            P("lat", "lon"),
            P(None, None, None, "lon", "lat"),
            P(None, "lon", "lat"),
            P(),
        ),
        out_specs=(
            P(None, None, None, "lat", "lon"),
            P(None, None, None, "lon", "lat"),
            P("lon", "lat", None),
        ),
        check_vma=False,
    )
```

```python
import functools

import jax
import jax.numpy as jnp
from jax import lax
from jax.experimental import pallas as pl
from jax.experimental.pallas import tpu as pltpu
from jax.sharding import PartitionSpec as P

SUB = 4
CELLS_DEV = 128
GLON_DEV = 4
DIFFUSE_ALONG = 0.3
DIFFUSE_ACROSS = 0.1
PAD = 4
CHUNK = 10
VMEM_GRANT = 12 << 20


class Sizes:
    def __init__(self, state_shape):
        self.nv, self.lev, self.wid, self.rows, self.cells = state_shape
        self.lanes = self.nv * self.lev
        self.half = self.cells // 2
        self.span = self.half + 2 * SUB + 2 * PAD
        self.group = 2 * self.rows
        self.wr = self.wid * self.rows
        self.packed = self.wr + self.rows
        self.packet = SUB * self.packed


def turned_courant(sz, ref, r):
    one = ref[pl.ds(r, sz.lev, stride=sz.rows), :]
    return jnp.concatenate([one] * sz.nv, axis=0).T


def put_halves(sz, out_ref, base, r, tile_ref, at):
    n = sz.half + SUB
    first = (base + PAD + SUB) * sz.group + r
    out_ref[pl.ds(first, n, stride=sz.group), :] = tile_ref[at : at + n, :]
    second = (base + PAD) * sz.group + sz.rows + r
    out_ref[pl.ds(second, n, stride=sz.group), :] = tile_ref[
        at + sz.half - SUB : at + sz.cells, :
    ]


def turn_in(sz, lat_two, lat_count, length_ref, z_ref, zc_ref, m_ref, mc_ref, mix_ref,
            zt_ref, zct_ref, mt_ref, mct_ref, w_ref, zfirst, zlast, ht, htp, mlow, mhigh,
            tile, low, high, z_in, zc_in, m_in, mc_in, mix_in, length, sems):
    copies = [
        pltpu.make_async_copy(source, target, sems.at[n])
        for n, (source, target) in enumerate((
            (length_ref, length), (m_ref, m_in), (mc_ref, mc_in), (z_ref, z_in),
            (zc_ref, zc_in), (mix_ref, mix_in),
        ))
    ]
    for copy in copies:
        copy.start()
    lon = lax.axis_index("lon")
    lat = lax.axis_index("lat")
    last = lat_count - 1
    edge = 8
    tile[0:edge, :] = jnp.zeros((edge, sz.lanes), jnp.float32)
    tile[edge + sz.cells :, :] = jnp.zeros((edge, sz.lanes), jnp.float32)
    owns_head = jnp.where(lon == 0, 1.0, 0.0).astype(jnp.float32)

    def place_tile(value, slot, r, base, out_ref, zonal):
        tile[edge : edge + sz.cells, :] = value
        put_halves(sz, out_ref, base, r, tile, edge)
        at = pl.ds(slot, SUB, stride=sz.packed)
        begin = tile[edge : edge + SUB, :]
        finish = tile[edge + sz.cells - SUB : edge + sz.cells, :]
        if zonal:
            zfirst[at, :] = begin
            zlast[at, :] = finish
            offset = jnp.clip(length[r] - SUB - lon * sz.cells, -SUB, sz.cells)
            ends = tile[pl.ds(edge + offset, SUB), :]
            ht[at, :] = begin * owns_head
            ht[pl.ds(sz.packet + slot, SUB, stride=sz.packed), :] = ends
        else:
            low[at, :] = begin
            high[at, :] = finish

    for zonal, s_ref, c_ref, st_ref, ct_ref in (
        (False, m_in, mc_in, mt_ref, mct_ref), (True, z_in, zc_in, zt_ref, zct_ref)
    ):
        if zonal:
            copies[0].wait()
            copies[3].wait()
            copies[4].wait()
        else:
            copies[1].wait()
            copies[2].wait()
        for r in range(sz.rows):
            for w in range(sz.wid):
                slot = w * sz.rows + r
                value = s_ref[pl.ds(slot, sz.lanes, stride=sz.wr), :].T
                place_tile(value, slot, r, w * sz.span, st_ref, zonal)
            place_tile(turned_courant(sz, c_ref, r), sz.wr + r, r, 0, ct_ref, zonal)
    htp[0 : 2 * sz.packet, :] = ht[...]
    north = jnp.where(lat == last, 1, 0)
    lows = low[...]
    highs = high[...]
    htp[2 * sz.packet :, :] = jnp.where(north == 1, highs, lows)
    if lat_two:
        mlow[...] = jnp.where(north == 1, lows, highs)
        mhigh[...] = jnp.zeros(mhigh.shape, jnp.float32)
    else:
        mlow[...] = lows
        mhigh[...] = highs
    copies[5].wait()
    turned = mix_in[...].T
    full = jnp.concatenate([turned] * sz.nv, axis=0)
    shape = (sz.lanes, sz.lanes)
    source = lax.broadcasted_iota(jnp.int32, shape, 0)
    target = lax.broadcasted_iota(jnp.int32, shape, 1)
    full = jnp.where(source // sz.lev == target // sz.lev, full, 0.0)
    stay = 1.0 - 2.0 * DIFFUSE_ALONG - 2.0 * DIFFUSE_ACROSS
    full = full + jnp.where(source == target, stay, 0.0)
    coarse = full.astype(jnp.bfloat16)
    fine = (full - coarse.astype(jnp.float32)).astype(jnp.bfloat16)
    w_ref[0 : sz.lanes, 0 : sz.lanes] = coarse
    w_ref[sz.lanes :, 0 : sz.lanes] = coarse
    w_ref[0 : sz.lanes, sz.lanes :] = fine
    w_ref[sz.lanes :, sz.lanes :] = fine


def combine(count, packet, *refs):
    own, zfirst, zlast = refs[:3]
    parts = refs[3 : 3 + count]
    total_ref, first_ref, last_ref = refs[3 + count :]
    total = own[0 : 2 * packet, :]
    for part in parts:
        total = total + part[0 : 2 * packet, :]
    total_ref[...] = total
    first_ref[0 : 2 * packet, :] = total
    first_ref[2 * packet :, :] = zfirst[...]
    last_ref[0 : 2 * packet, :] = total
    last_ref[2 * packet :, :] = zlast[...]


def substeps(sz, w_ref, a_ref, b_ref, ca_ref, cb_ref, courant_ref):
    lo_y = PAD * sz.group
    rows = (sz.half + 2 * SUB) * sz.group
    c = courant_ref[lo_y : lo_y + rows, :]
    ca_ref[lo_y : lo_y + rows, :] = DIFFUSE_ALONG - 0.5 * c
    cb_ref[lo_y : lo_y + rows, :] = DIFFUSE_ALONG + 0.5 * c
    g = sz.group

    def step(src, dst):
        total = sz.half + 2 * SUB - 2
        for begin in range(0, total, CHUNK):
            size = min(CHUNK, total - begin)
            y = PAD + 1 + begin
            n = size * g
            here = [src[(w * sz.span + y) * g : (w * sz.span + y) * g + n, :] for w in range(sz.wid)]
            stacked = jnp.concatenate(here, axis=0)
            coarse = stacked.astype(jnp.bfloat16)
            fine = (stacked - coarse.astype(jnp.float32)).astype(jnp.bfloat16)
            product = jnp.dot(
                jnp.concatenate([coarse, fine], axis=1), w_ref[...],
                preferred_element_type=jnp.float32,
            )
            ca = ca_ref[y * g : y * g + n, :]
            cb = cb_ref[y * g : y * g + n, :]
            for w in range(sz.wid):
                at = (w * sz.span + y) * g
                up = here[min(w + 1, sz.wid - 1)]
                down = here[max(w - 1, 0)]
                part = product[w * n : (w + 1) * n]
                value = part[:, : sz.lanes] + part[:, sz.lanes :]
                value = value + DIFFUSE_ACROSS * (up + down)
                value = value + src[at + g : at + g + n, :] * ca
                value = value + src[at - g : at - g + n, :] * cb
                dst[at : at + n, :] = value

    def pair(_, carry):
        step(a_ref, b_ref)
        step(b_ref, a_ref)
        return carry

    lax.fori_loop(0, SUB // 2, pair, 0)


def merid_kernel(sz, lat_two, lat_count, mt, mct, w_ref, pole, lat_a, lat_b, own_b, out_ref,
                 b_ref, ca_ref, cb_ref, ct_ref):
    lat = lax.axis_index("lat")
    last = lat_count - 1
    out_ref[...] = mt[...]
    ct_ref[...] = mct[...]
    base = 2 * sz.packet
    for d in range(SUB):
        for slot in range(sz.packed):
            courant = slot >= sz.wr
            w, r = divmod(slot, sz.rows)
            partner = slot if courant else (sz.wid - 1 - w) * sz.rows + r
            sign = -1.0 if courant else 1.0
            ref = ct_ref if courant else out_ref
            begin = 0 if courant else w * sz.span
            mirrored = (SUB - 1 - d) * sz.packed + partner
            over = sign * pole[base + mirrored : base + mirrored + 1, :]
            at = d * sz.packed + slot
            south = jnp.where(lat == 0, over, lat_a[at : at + 1, :])
            north = jnp.where(lat == last, over, lat_b[at : at + 1, :])
            row = (begin + PAD + d) * sz.group + r
            ref[row : row + 1, :] = south
            row = (begin + PAD + SUB + sz.half + d) * sz.group + sz.rows + r
            ref[row : row + 1, :] = north
    substeps(sz, w_ref, out_ref, b_ref, ca_ref, cb_ref, ct_ref)


def zonal_kernel(sz, shift_count, length_ref, owner_ref, zt, zct, w_ref, own, behind, ahead, *refs):
    others = refs[:shift_count]
    out_ref, below_ref, mid_ref, above_ref, b_ref, ca_ref, cb_ref, ct_ref, length, owner, sems = (
        refs[shift_count:]
    )
    copies = [
        pltpu.make_async_copy(length_ref, length, sems.at[0]),
        pltpu.make_async_copy(owner_ref, owner, sems.at[1]),
    ]
    for copy in copies:
        copy.start()
    lon = lax.axis_index("lon")
    out_ref[...] = zt[...]
    ct_ref[...] = zct[...]
    ends = own[...] + behind[0 : 2 * sz.packet, :] + ahead[0 : 2 * sz.packet, :]
    for other in others:
        ends = ends + other[...]
    head = ends[: sz.packet]
    left = jnp.where(lon == 0, ends[sz.packet :], behind[2 * sz.packet :, :])
    right = ahead[2 * sz.packet :, :]
    for d in range(SUB):
        for slot in range(sz.packed):
            courant = slot >= sz.wr
            w, r = divmod(slot, sz.rows)
            ref = ct_ref if courant else out_ref
            r = slot % sz.rows
            begin = 0 if courant else w * sz.span
            at = d * sz.packed + slot
            row = (begin + PAD + d) * sz.group + r
            ref[row : row + 1, :] = left[at : at + 1]
            row = (begin + PAD + SUB + sz.half + d) * sz.group + sz.rows + r
            ref[row : row + 1, :] = right[at : at + 1]
    copies[0].wait()
    for r in range(sz.rows):
        past = length[r] - lon * sz.cells
        for h in range(2):
            y = jnp.clip(past + PAD + SUB - h * sz.half, 0, sz.span - SUB)
            for slot in range(r, sz.packed, sz.rows):
                courant = slot >= sz.wr
                ref = ct_ref if courant else out_ref
                begin = 0 if courant else (slot // sz.rows) * sz.span
                for d in range(SUB):
                    at = d * sz.packed + slot
                    row = (begin + y + d) * sz.group + h * sz.rows + r
                    ref[pl.ds(row, 1), :] = head[at : at + 1]
    substeps(sz, w_ref, out_ref, b_ref, ca_ref, cb_ref, ct_ref)
    scale = GLON_DEV / (3.0 * CELLS_DEV)
    near = 8
    copies[1].wait()
    for r in range(sz.rows):
        column = lon * GLON_DEV - 1 + lax.broadcasted_iota(jnp.int32, (near, sz.cells), 0)
        cell = lon * sz.cells + lax.broadcasted_iota(jnp.int32, (near, sz.cells), 1)
        own_row = owner[r : r + 1, :]
        table = jnp.where((own_row == column) & (cell < length[r]), 1.0, 0.0)
        halves = []
        for h in range(2):
            change = None
            for w in range(sz.wid):
                at = pl.ds((w * sz.span + PAD + SUB) * sz.group + h * sz.rows + r,
                           sz.half, stride=sz.group)
                part = out_ref[at, :] - zt[at, :]
                change = part if change is None else change + part
            halves.append(change)
        change = jnp.concatenate(halves, axis=0) * scale
        sums = jnp.dot(
            table.astype(jnp.float32), change, precision=lax.Precision.HIGHEST,
            preferred_element_type=jnp.float32,
        )
        below_ref[r : r + 1, :] = sums[0:1]
        above_ref[r : r + 1, :] = sums[GLON_DEV + 1 : GLON_DEV + 2]
        for g in range(GLON_DEV):
            mid_ref[g * sz.rows + r : g * sz.rows + r + 1, :] = sums[g + 1 : g + 2]


def turn_out(sz, length_ref, z_ref, mt, zt, m_out, z_out, m_own, z_own, length, sems):
    reads = [pltpu.make_async_copy(length_ref, length, sems.at[0])]
    for copy in reads:
        copy.start()
    writes = []
    lon = lax.axis_index("lon")
    cell = lon * sz.cells + lax.broadcasted_iota(jnp.int32, (sz.lanes, sz.cells), 1)
    for zonal, src, dst, out in ((False, mt, m_own, m_out), (True, zt, z_own, z_out)):
        if zonal:
            for copy in reads:
                copy.wait()
        for w in range(sz.wid):
            for r in range(sz.rows):
                halves = [
                    src[pl.ds((w * sz.span + PAD + SUB) * sz.group + h * sz.rows + r,
                              sz.half, stride=sz.group), :]
                    for h in range(2)
                ]
                value = jnp.concatenate(halves, axis=0).T
                at = pl.ds(w * sz.rows + r, sz.lanes, stride=sz.wr)
                if zonal:
                    value = jnp.where(cell < length[r], value, z_ref[at, :])
                dst[at, :] = value
        writes.append(pltpu.make_async_copy(dst, out, sems.at[1 + zonal]))
        writes[-1].start()
    for copy in writes:
        copy.wait()


def finish(sz, mid, from_left, from_right, out_ref):
    end = (GLON_DEV - 1) * sz.rows
    out_ref[0 : sz.rows, :] = mid[0 : sz.rows, :] + from_left[...]
    out_ref[sz.rows : end, :] = mid[sz.rows : end, :]
    out_ref[end:, :] = mid[end:, :] + from_right[...]


def call(body, outs, spaces, scratch=(), name=None, flops=1 << 20, out_space=pltpu.VMEM):
    return pl.pallas_call(
        body,
        out_shape=outs,
        in_specs=[pl.BlockSpec(memory_space=space) for space in spaces],
        out_specs=[pl.BlockSpec(memory_space=out_space)] * len(outs),
        scratch_shapes=list(scratch),
        compiler_params=pltpu.CompilerParams(vmem_limit_bytes=VMEM_GRANT),
        cost_estimate=pl.CostEstimate(flops=flops, bytes_accessed=4 << 20, transcendentals=0),
        name=name,
    )


def shifted(value, axis, steps):
    count = lax.axis_size(axis)
    return lax.ppermute(value, axis, [(i, (i + steps) % count) for i in range(count)])


def shards(
    zonal_state, zonal_courant, zonal_length, zonal_owner, merid_state, merid_courant, mixing
):
    sz = Sizes(zonal_state.shape)
    zonal_length = pltpu.with_memory_space_constraint(zonal_length, pltpu.HBM)
    f32 = lambda *shape: jax.ShapeDtypeStruct(shape, jnp.float32)
    lon_count = lax.axis_size("lon")
    lat_count = lax.axis_size("lat")
    lat_two = lat_count == 2
    flat = lambda a: a.reshape(-1, sz.cells)
    hbm = lambda a: pltpu.with_memory_space_constraint(a, pltpu.HBM)
    z, m = hbm(flat(zonal_state)), hbm(flat(merid_state))
    state_rows = sz.wid * sz.span * sz.group
    courant_rows = sz.span * sz.group
    packet = sz.packet
    lanes = sz.lanes
    zt, zct, mt, mct, weights, zfirst, zlast, ht, htp, mlow, mhigh = call(
        functools.partial(turn_in, sz, lat_two, lat_count),
        (
            f32(state_rows, lanes), f32(courant_rows, lanes),
            f32(state_rows, lanes), f32(courant_rows, lanes),
            jax.ShapeDtypeStruct((2 * lanes, 2 * lanes), jnp.bfloat16),
            f32(packet, lanes), f32(packet, lanes), f32(2 * packet, lanes),
            f32(3 * packet, lanes), f32(packet, lanes), f32(packet, lanes),
        ),
        [pltpu.HBM] * 6,
        (
            pltpu.VMEM((sz.cells + 16, lanes), jnp.float32),
            pltpu.VMEM((packet, lanes), jnp.float32),
            pltpu.VMEM((packet, lanes), jnp.float32),
            pltpu.VMEM(z.shape, jnp.float32),
            pltpu.VMEM((sz.lev * sz.rows, sz.cells), jnp.float32),
            pltpu.VMEM(m.shape, jnp.float32),
            pltpu.VMEM((sz.lev * sz.rows, sz.cells), jnp.float32),
            pltpu.VMEM((lanes, sz.lev), jnp.float32),
            pltpu.SMEM((sz.rows,), jnp.int32),
            pltpu.SemaphoreType.DMA((6,)),
        ),
        "turn_in",
    )(zonal_length, z, hbm(flat(zonal_courant)), m, hbm(flat(merid_courant)),
      hbm(mixing.reshape(lanes, sz.lev)))
    pole = shifted(htp, "lon", lon_count // 2)
    if lat_two:
        lat_a = lat_b = shifted(mlow, "lat", 1)
    else:
        lat_b = shifted(mlow, "lat", -1)
        lat_a = shifted(mhigh, "lat", 1)
    stride = lon_count
    own = ht
    stages = []
    while stride > 4:
        radix = 4 if stride % 16 == 0 and stride != lon_count * 2 else 2
        stages.append((stride // radix, radix))
        stride //= radix
    for number, (width, radix) in enumerate(stages):
        parts = []
        for s in range(1, radix):
            if number == 0 and s * width == lon_count // 2:
                parts.append(pole)
            else:
                parts.append(shifted(own, "lon", s * width))
        own, to_left, to_right = call(
            functools.partial(combine, len(parts), packet),
            (f32(2 * packet, lanes), f32(3 * packet, lanes), f32(3 * packet, lanes)),
            [pltpu.VMEM] * (3 + len(parts)), (), "combine",
        )(own, zfirst, zlast, *parts)
    behind = shifted(to_right, "lon", 1)
    ahead = shifted(to_left, "lon", -1)
    others = [shifted(own, "lon", s) for s in range(2, stride - 1)]
    work = (
        pltpu.VMEM((state_rows, lanes), jnp.float32),
        pltpu.VMEM((courant_rows, lanes), jnp.float32),
        pltpu.VMEM((courant_rows, lanes), jnp.float32),
        pltpu.VMEM((courant_rows, lanes), jnp.float32),
    )
    (mt_next,) = call(
        functools.partial(merid_kernel, sz, lat_two, lat_count),
        (f32(state_rows, lanes),), [pltpu.VMEM] * 7, work, "merid", 1 << 32,
    )(mt, mct, weights, pole, lat_a, lat_b, mhigh)
    own, mt_next = lax.optimization_barrier((own, mt_next))
    zt_next, below, mid, above = call(
        functools.partial(zonal_kernel, sz, len(others)),
        (
            f32(state_rows, lanes), f32(sz.rows, lanes), f32(GLON_DEV * sz.rows, lanes),
            f32(sz.rows, lanes),
        ),
        [pltpu.HBM] * 2 + [pltpu.VMEM] * (6 + len(others)),
        work + (
            pltpu.SMEM((sz.rows,), jnp.int32),
            pltpu.VMEM((sz.rows, sz.cells), jnp.int32),
            pltpu.SemaphoreType.DMA((2,)),
        ),
        "zonal", 1 << 32,
    )(zonal_length, zonal_owner, zt, zct, weights, own, behind, ahead, *others)
    from_right = shifted(below, "lon", -1)
    from_left = shifted(above, "lon", 1)
    m_next, z_next = call(
        functools.partial(turn_out, sz),
        (f32(*m.shape), f32(*z.shape)), [pltpu.HBM] + [pltpu.VMEM] * 3,
        (
            pltpu.VMEM(m.shape, jnp.float32), pltpu.VMEM(z.shape, jnp.float32),
            pltpu.SMEM((sz.rows,), jnp.int32), pltpu.SemaphoreType.DMA((3,)),
        ),
        "turn_out", 1 << 32, pltpu.HBM,
    )(zonal_length, flat(zonal_state), mt_next, zt_next)
    (coupling,) = call(
        functools.partial(finish, sz), (f32(*mid.shape),), [pltpu.VMEM] * 3, (), "finish",
    )(mid, from_left, from_right)
    coupling = coupling.reshape(GLON_DEV, sz.rows, lanes)
    return z_next.reshape(zonal_state.shape), m_next.reshape(merid_state.shape), coupling


def solution(mesh):
    return jax.shard_map(
        shards,
        mesh=mesh,
        in_specs=(
            P(None, None, None, "lat", "lon"),
            P(None, "lat", "lon"),
            P("lat"),
            P("lat", "lon"),
            P(None, None, None, "lon", "lat"),
            P(None, "lon", "lat"),
            P(),
        ),
        out_specs=(
            P(None, None, None, "lat", "lon"),
            P(None, None, None, "lon", "lat"),
            P("lon", "lat", None),
        ),
        check_vma=False,
    )
```
